32 devices in a mesh: rows: 4 (over z), vocab: 8 (over y, x, core).
Axes of the slice: x: 2, y: 2, z: 4, core: 2. Of those that a mesh axis runs over, the one named last changes fastest.
Arguments:
- hidden: bfloat16 [512, 8192], P('rows', 'vocab'), may hold values from -30 to 30
- head: bfloat16 [8192, 152064], P(None, ('vocab', 'rows')), may hold values from -1 to 1
- states: int32 [512], replicated, may hold values from 0 to 2047
- class_of: int32 [152064], P('vocab'), may hold values from 0 to 255, as said below
- table: int32 [2048, 8], replicated, may hold values from -2147483648 to 2147483646, as said below
Outputs:
- log_probs: float32 [512, 152064], P('rows', 'vocab')
- entropy: float32 [512], P('rows')
The draws below stay inside these ranges and needn't reach their ends.
Inputs may be any that keep to these rules, and one draw needn't show every extreme that they name: `class_of`: class 0 is the class of at least one token. `table`: bit 0 of word 0 is set in every state, so class 0 is allowed everywhere.
All inputs are finite; a program needn't handle non-finite values.
Results may differ from the reference program's by a relative error of at most 0.0003.
Values may be sent and summed in bfloat16 or wider, within the bound.
A program may use at most 192 MiB of HBM per device.

```python
import jax
import jax.numpy as jnp
from jax import lax

D = 8192
V = 152064
STATES = 2048
CLASSES = 256
ROWS = 512


def head_block(key, index):
    block_key = jax.random.fold_in(jax.random.fold_in(key, 101), index)
    values = jax.random.normal(block_key, (D, V // 64), jnp.float32) * D ** (-0.5)
    return jnp.clip(values, -1.0, 1.0)


def special_pairs(key):
    base = jax.random.fold_in(key, 103)
    blocks = jax.random.randint(jax.random.fold_in(base, 1), (6,), 0, 64)
    first = jax.random.randint(jax.random.fold_in(base, 2), (6,), 0, V // 64)
    offset = jax.random.randint(jax.random.fold_in(base, 3), (6,), 1, V // 64)
    second = (first + offset) % (V // 64)
    return (blocks, first, second)


def narrow_block(key):

    def build(index):
        return head_block(key, index).astype(jnp.bfloat16)
    return build


def draw_head(key, part):
    blocks = lax.map(narrow_block(key), jnp.arange(64, dtype=jnp.int32))
    return jnp.transpose(blocks, (1, 0, 2)).reshape(D, V).astype(jnp.bfloat16)


def draw_hidden(key, part):
    values = jax.random.normal(jax.random.fold_in(key, 201), (ROWS, D), jnp.float32) * 3.0
    values = jnp.clip(values, -18.0, 18.0)
    return jnp.clip(values, -30.0, 30.0).astype(jnp.bfloat16)


def draw_class_of(key, part):
    classes = jax.random.randint(jax.random.fold_in(key, 301), (V,), 0, CLASSES)
    blocks, first, second = special_pairs(key)
    width = V // 64
    classes = classes.at[blocks * width + first].set(0)
    classes = classes.at[blocks * width + second].set(0)
    return classes.astype(jnp.int32)


def draw_table(key, part):
    words = jax.random.randint(jax.random.fold_in(key, 401), (STATES, CLASSES // 32), -2147483648, 2147483647, jnp.int32)
    return words.at[:, 0].set(jnp.bitwise_or(words[:, 0], 1)).astype(jnp.int32)


def touch_ends(entries, key, smallest, top_value):
    longest = entries.shape.index(max(entries.shape))
    spots = []
    for shift in (0, 1):
        where = [jax.random.randint(jax.random.fold_in(key, axis), (), 0, length) for axis, length in enumerate(entries.shape)]
        where[longest] = (where[longest] + shift) % entries.shape[longest]
        spots.append(tuple(where))
    return entries.at[spots[0]].set(smallest).at[spots[1]].set(top_value)


def setup_inputs(seed: int = 0) -> dict:
    seeds = jax.random.split(jax.random.key(seed), 6)
    hidden = draw_hidden(jax.random.fold_in(seeds[5], 71), 0)
    head = draw_head(jax.random.fold_in(seeds[5], 71), 0)
    states = touch_ends(jax.random.randint(seeds[2], (ROWS,), 0, STATES), jax.random.fold_in(seeds[2], 1), 0, STATES - 1).astype(jnp.int32)
    class_of = draw_class_of(jax.random.fold_in(seeds[5], 71), 0)
    table = draw_table(jax.random.fold_in(seeds[5], 71), 0)
    return {"hidden": hidden, "head": head, "states": states, "class_of": class_of, "table": table}


def reference(hidden, head, states, class_of, table):
    logits = jnp.dot(hidden, head, preferred_element_type=jnp.float32)
    words = jnp.take(table, states, axis=0)
    shifts = jnp.arange(32, dtype=jnp.int32)
    bit_values = jnp.bitwise_and(jnp.right_shift(words[:, :, None], shifts[None, None, :]), 1)
    allowed_class = bit_values.reshape(words.shape[0], words.shape[1] * 32)
    allowed = jnp.take(allowed_class, class_of, axis=1) > 0
    peak = jnp.max(jnp.where(allowed, logits, -1.0e30), axis=1)
    weights = jnp.where(allowed, jnp.exp(logits - peak[:, None]), 0.0)
    total = jnp.sum(weights, axis=1)
    weighted = jnp.sum(weights * logits, axis=1)
    norm_log = peak + jnp.log(total)
    log_probs = jnp.where(allowed, logits - norm_log[:, None], 0.0)
    entropy = norm_log - weighted / total
    return log_probs, entropy
```

```python
import functools

import jax
import jax.numpy as jnp
from jax import lax
from jax.experimental import pallas as pl
from jax.experimental.pallas import tpu as pltpu
from jax.sharding import PartitionSpec as P

MESH = pl.DeviceIdType.MESH
LANES = 128
BIG = 1e30
LEVELS = 65000.0
SHIFT = 32500
FORBIDDEN = -32768
MAX_CHUNKS = 11
BUFFERS = 3
PIECES = 2
SUB = 144


def chunk_count(columns):
    for n in range(MAX_CHUNKS, 1, -1):
        if columns % n == 0 and (columns // n) % 16 == 0:
            return n
    return 1


def flip(v, bits):
    for bit in bits:
        size = 1 << bit
        v = v + size * (1 - 2 * lax.rem(lax.div(v, size), 2))
    return v


def subsets(bits):
    found = [()]
    for bit in bits:
        found = found + [s + (bit,) for s in found]
    return found


def exchange_kernel(
    nz, nv, hidden, head, states, class_of, table, codes_out, base_out, step_out, result,
    hid, buf, codes, banned, classes, onehot, x, scale_rows, scale_land, stat_own, stat_land,
    z_send, z_recv, f_send, h_send, h_recv, own_sem, head_sem, c_send, c_recv, s_send, s_recv, loc_sem, t_send, t_recv,
):
    rows, width = hidden.shape
    columns = head.shape[0]
    n = codes.shape[1]
    size = columns // n
    half = nz // 2
    piece = rows // PIECES
    steps = nv.bit_length() - 1
    z = lax.axis_index("rows")
    v = lax.axis_index("vocab")
    side = lax.div(z, half)
    far_base = (1 - side) * half
    near_base = side * half

    def send(src, dst, ssem, rsem, zz, vv):
        return pltpu.make_async_remote_copy(
            src_ref=src, dst_ref=dst, send_sem=ssem, recv_sem=rsem, device_id=(zz, vv), device_id_type=MESH
        )

    def z_peer(j):
        return lax.rem(z + j, nz)

    def v_peer(j):
        return lax.rem(v + j, nv)

    barrier = pltpu.get_barrier_semaphore()
    for j in range(1, nz):
        pl.semaphore_signal(barrier, inc=1, device_id=(z_peer(j), v), device_id_type=MESH)
    for j in range(1, nv):
        pl.semaphore_signal(barrier, inc=1, device_id=(z, v_peer(j)), device_id_type=MESH)

    def head_copy(t):
        at = lax.rem(t, BUFFERS)
        start = pl.multiple_of(lax.rem(t, n) * size, 16) if n > 1 else 0
        return pltpu.make_async_copy(head.at[pl.ds(start, size), :], buf.at[at], head_sem.at[at])

    for t in range(min(BUFFERS, 2 * n)):
        head_copy(jnp.int32(t)).start()

    pl.semaphore_wait(barrier, nz - 1 + nv - 1)

    def slot(zz, p, vv):
        return hid.at[zz, pl.ds(p * piece, piece), pl.ds(pl.multiple_of(vv * width, width), width)]

    def own(p):
        return hidden.at[pl.ds(p * piece, piece), :]

    def far(k):
        return (1 - side) * (half + k) + side * (half - 1 - k)

    def near(j):
        return near_base + lax.rem(z - near_base + j, half)

    inner = (1 - side) * half + side * (half - 1)
    outward = jnp.clip(z - 1 + 2 * side, 0, nz - 1)
    outermost = side * (nz - 1)

    def cross(p):
        return send(own(p), slot(z, p, v), z_send.at[0, p], z_recv.at[z, p], inner, v)

    def beside(j, p):
        return send(own(p), slot(z, p, v), z_send.at[j, p], z_recv.at[z, p], near(j), v)

    def onward(k, p):
        zz = far(k)
        return send(slot(zz, p, v), slot(zz, p, v), f_send.at[k, p], z_recv.at[zz, p], outward, v)

    def arrived(zz, p):
        send(slot(zz, p, v), slot(zz, p, v), z_send.at[0, p], z_recv.at[zz, p], z, v).wait_recv()

    for p in range(PIECES):
        cross(p).start()
    for j in range(1, half):
        for p in range(PIECES):
            beside(j, p).start()
    for p in range(PIECES):
        pltpu.make_async_copy(own(p), slot(z, p, v), own_sem.at[p]).start()

    def order(p):
        upper = list(range(1, steps))
        if p % 2:
            upper = upper[::-1]
        return upper + [0]

    def spread(q, zz, p, s, is_own):
        bits = order(p)
        partner = flip(v, [bits[s]])
        for m in subsets(bits[:s]):
            vv = flip(v, m)
            src = own(p) if (is_own and not m) else slot(zz, p, vv)
            send(src, slot(zz, p, vv), h_send.at[q, p, s], h_recv.at[q, p, s], z, partner).start()

    def spread_step(q, p, s):
        block = hid.at[0, pl.ds(p * piece, piece), pl.ds(0, width << s)]
        return send(block, block, h_send.at[q, p, s], h_recv.at[q, p, s], z, v)

    for zz in range(nz):
        @pl.when(z == zz)
        def _(zz=zz):
            classes[:, pl.ds(0, columns)] = class_of[:, zz * columns:(zz + 1) * columns]

    n_classes = onehot.shape[1]
    kinds = lax.broadcasted_iota(jnp.int32, (LANES, n_classes), 1)
    for b in range(-(-columns // LANES)):
        some = min(LANES, columns - b * LANES)
        line = classes[:, b * LANES:(b + 1) * LANES]
        turned = jnp.transpose(jnp.broadcast_to(line, (LANES, LANES)))
        wide = jnp.concatenate([turned] * (n_classes // LANES), axis=1)
        hot = jnp.where(wide == kinds, 1.0, 0.0).astype(jnp.bfloat16)
        onehot[b * LANES:b * LANES + some, :] = hot[:some]

    n_words, n_states = table.shape
    n_bytes = 4 * n_words
    packed = table[...]
    parts = [jnp.bitwise_and(jnp.right_shift(packed, 8 * b), 255) for b in range(4)]
    octets = jnp.concatenate(parts, axis=0).astype(jnp.float32).astype(jnp.bfloat16)
    which = lax.broadcasted_iota(jnp.int32, (n_states, rows), 0)
    bits8 = lax.broadcasted_iota(jnp.int32, (8, rows), 0)
    for g in range(nz):
        hot = jnp.where(which == states[:, g * rows:(g + 1) * rows], 1.0, 0.0).astype(jnp.bfloat16)
        found = jnp.dot(octets, hot, preferred_element_type=jnp.float32).astype(jnp.int32)
        blocks = []
        for w in range(n_words):
            for b in range(4):
                line = found[b * n_words + w:b * n_words + w + 1, :]
                bit = jnp.bitwise_and(jnp.right_shift(jnp.broadcast_to(line, (8, rows)), bits8), 1)
                blocks.append(jnp.where(bit > 0, 0.0, -BIG))
        banned[g] = jnp.concatenate(blocks, axis=0).astype(jnp.bfloat16)

    def running(g):
        return scale_rows.at[g, pl.ds(2 * n, 8), :]

    for g in range(nz):
        first = lax.broadcasted_iota(jnp.int32, (8, rows), 0) == 0
        scale_rows[g, 2 * n:2 * n + 8, :] = jnp.where(first, -BIG, 0.0)

    for k in range(half):
        for p in range(PIECES):
            arrived(far(k), p)

            @pl.when(z != outermost)
            def _(k=k, p=p):
                onward(k, p).start()

            spread(k, far(k), p, 0, False)
    for s in range(1, steps):
        for k in range(half):
            for p in range(PIECES):
                spread_step(k, p, s - 1).wait_recv()
                spread(k, far(k), p, s, False)

    def near_event(s):
        for j in range(half):
            for p in range(PIECES):
                if s > 0:
                    spread_step(half + j, p, s - 1).wait_recv()
                elif j == 0:
                    pltpu.make_async_copy(own(p), slot(z, p, v), own_sem.at[p]).wait()
                else:
                    arrived(near(j), p)
                if s < steps:
                    spread(half + j, near(j), p, s, j == 0)

    near_event(0)
    for k in range(half):
        for p in range(PIECES):
            spread_step(k, p, steps - 1).wait_recv()

    n_rows = half * rows

    def encode(g, i, lanes):
        values = x[:, lanes]
        high = jnp.max(values, axis=0, keepdims=True)
        low = jnp.min(jnp.where(values > -0.1 * BIG, values, BIG), axis=0, keepdims=True)
        gap = jnp.maximum(high - low, 1e-30)
        rate = LEVELS / gap
        total = jnp.zeros((1, rows), jnp.float32)
        weighted = jnp.zeros((1, rows), jnp.float32)
        for r in range(0, size, SUB):
            end = min(r + SUB, size)
            values = x[r:end, lanes]
            level = jnp.maximum((values - low) * rate + 0.5, float(FORBIDDEN + SHIFT))
            codes[g, i, r:end, :] = (level.astype(jnp.int32) - SHIFT).astype(jnp.int16)
            weights = jnp.exp(values - high)
            total = total + jnp.sum(weights, axis=0, keepdims=True)
            weighted = weighted + jnp.sum(weights * values, axis=0, keepdims=True)
        step = gap * (1.0 / LEVELS)
        scale_rows[g, pl.ds(i, 1), :] = low + SHIFT * step
        scale_rows[g, pl.ds(n + i, 1), :] = step
        old = scale_rows[g, 2 * n:2 * n + 3, :]
        peak = jnp.maximum(old[0:1], high)
        f0 = jnp.exp(old[0:1] - peak)
        f1 = jnp.exp(high - peak)
        scale_rows[g, 2 * n:2 * n + 1, :] = peak
        scale_rows[g, 2 * n + 1:2 * n + 2, :] = f0 * old[1:2] + f1 * total
        scale_rows[g, 2 * n + 2:2 * n + 3, :] = f0 * old[2:3] + f1 * weighted

    def code_copy(g, i):
        return send(codes.at[g, i], codes_out.at[z, i], c_send.at[g], c_recv.at[z], g, v)

    def scale_copy(g):
        return send(scale_rows.at[g], scale_land.at[z], s_send.at[g], s_recv.at[z], g, v)

    def run_pass(index, base, events):
        def chunk_step(i, carry):
            t = index * n + i
            for e, event in enumerate(events):
                @pl.when(i == min(2 * e + 1, n - 1))
                def _(event=event):
                    event()
            head_copy(t).wait()
            weights = hid[pl.ds(base, half)].reshape(n_rows, hid.shape[2])
            got = lax.dot_general(
                buf[lax.rem(t, BUFFERS)], weights, (((1,), (1,)), ((), ())), preferred_element_type=jnp.float32
            )
            mine = onehot[pl.ds(pl.multiple_of(i * size, 16) if n > 1 else 0, size), :]
            for j in range(half):
                x[:, j * rows:(j + 1) * rows] = got[:, j * rows:(j + 1) * rows] + jnp.dot(
                    mine, banned[base + j], preferred_element_type=jnp.float32
                )

            @pl.when(t + BUFFERS < 2 * n)
            def _():
                head_copy(t + BUFFERS).start()

            for j in range(half):
                encode(base + j, i, slice(j * rows, (j + 1) * rows))
            for j in range(half):
                g = base + j
                if index == 0:
                    code_copy(g, i).start()
                else:
                    @pl.when(g != z)
                    def _(g=g):
                        code_copy(g, i).start()

                    @pl.when(g == z)
                    def _(g=g):
                        pltpu.make_async_copy(codes.at[g, i], codes_out.at[z, i], loc_sem).start()
            return carry

        lax.fori_loop(0, n, chunk_step, 0)
        for j in range(half):
            g = base + j
            if index == 0:
                scale_copy(g).start()
            else:
                @pl.when(g != z)
                def _(g=g):
                    scale_copy(g).start()

    run_pass(0, far_base, [functools.partial(near_event, s) for s in range(1, steps + 1)])
    run_pass(1, near_base, [])
    scale_land[z] = scale_rows[z]

    for j in range(1, nz):
        g = z_peer(j)
        send(scale_rows.at[g], scale_land.at[g], s_send.at[g], s_recv.at[g], z, v).wait_recv()

    def combine(ref, count, line):
        peaks, totals, weights = [
            jnp.concatenate([ref[q, line + k:line + k + 1, :] for q in range(count)], axis=0) for k in range(3)
        ]
        peak = jnp.max(peaks, axis=0, keepdims=True)
        factor = jnp.exp(peaks - peak)
        return (
            peak,
            jnp.sum(factor * totals, axis=0, keepdims=True),
            jnp.sum(factor * weights, axis=0, keepdims=True),
        )

    def stat_copy(j):
        return send(stat_own, stat_land.at[v], t_send.at[j], t_recv.at[v], z, v_peer(j))

    summed = jnp.concatenate([*combine(scale_land, nz, 2 * n), jnp.zeros((5, rows), jnp.float32)], axis=0)
    stat_own[...] = summed
    stat_land[v] = summed
    for j in range(1, nv):
        stat_copy(j).start()
    for j in range(1, nv):
        u = v_peer(j)
        send(stat_own, stat_land.at[u], t_send.at[j], t_recv.at[u], z, v).wait_recv()
    peak, total, weighted = combine(stat_land, nv, 0)
    norm = peak + jnp.log(total)
    result[...] = norm - weighted / total
    for g in range(nz):
        base_out[g] = scale_land[g, 0:n, :] - norm
        step_out[g] = scale_land[g, n:2 * n, :]

    for j in range(1, nz):
        g = z_peer(j)
        whole = send(codes.at[g], codes_out.at[g], c_send.at[g], c_recv.at[g], z, v)
        whole.wait_send()
        whole.wait_recv()
        scale_copy(g).wait_send()
    pltpu.make_async_copy(codes.at[z], codes_out.at[z], loc_sem).wait()
    for j in range(1, nv):
        stat_copy(j).wait_send()
    for p in range(PIECES):
        cross(p).wait_send()
        for j in range(1, half):
            beside(j, p).wait_send()

        @pl.when(z != outermost)
        def _(p=p):
            for k in range(half):
                onward(k, p).wait_send()

        for q in range(nz):
            for s in range(steps):
                spread_step(q, p, s).wait_send()


def exchange(nz, nv, hidden, head, states, class_of, table):
    rows, width = hidden.shape
    columns, depth = head.shape
    n = chunk_count(columns)
    size = columns // n
    lines = -(-(2 * n + 8) // 8) * 8
    steps = nv.bit_length() - 1
    half = nz // 2
    padded = -(-columns // LANES) * LANES
    n_classes = table.shape[0] * 32
    vmem = pl.BlockSpec(memory_space=pltpu.VMEM)
    hbm = pl.BlockSpec(memory_space=pl.ANY)
    dma = pltpu.SemaphoreType.DMA
    return pl.pallas_call(
        functools.partial(exchange_kernel, nz, nv),
        out_shape=[
            jax.ShapeDtypeStruct((nz, n, size, rows), jnp.int16),
            jax.ShapeDtypeStruct((nz, n, rows), jnp.float32),
            jax.ShapeDtypeStruct((nz, n, rows), jnp.float32),
            jax.ShapeDtypeStruct((1, rows), jnp.float32),
        ],
        in_specs=[vmem, hbm, vmem, vmem, vmem],
        out_specs=[hbm, vmem, vmem, vmem],
        scratch_shapes=[
            pltpu.VMEM((nz, rows, depth), jnp.bfloat16),
            pltpu.VMEM((BUFFERS, size, depth), jnp.bfloat16),
            pltpu.VMEM((nz, n, size, rows), jnp.int16),
            pltpu.VMEM((nz, n_classes, rows), jnp.bfloat16),
            pltpu.VMEM((1, padded), jnp.int32),
            pltpu.VMEM((columns, n_classes), jnp.bfloat16),
            pltpu.VMEM((size, half * rows), jnp.float32),
            pltpu.VMEM((nz, lines, rows), jnp.float32),
            pltpu.VMEM((nz, lines, rows), jnp.float32),
            pltpu.VMEM((8, rows), jnp.float32),
            pltpu.VMEM((nv, 8, rows), jnp.float32),
            dma((half, PIECES)),
            dma((nz, PIECES)),
            dma((half, PIECES)),
            dma((nz, PIECES, steps)),
            dma((nz, PIECES, steps)),
            dma((PIECES,)),
            dma((BUFFERS,)),
            dma((nz,)),
            dma((nz,)),
            dma((nz,)),
            dma((nz,)),
            dma,
            dma((nv,)),
            dma((nv,)),
        ],
        compiler_params=pltpu.CompilerParams(
            collective_id=0, has_side_effects=True, vmem_limit_bytes=62 * 1024 * 1024
        ),
    )(hidden, head, states, class_of, table)


def solution(mesh):
    nz, nv = mesh.shape["rows"], mesh.shape["vocab"]

    def on_device(hidden, head, states, class_of, table):
        codes, base, step, entropy = exchange(
            nz, nv, hidden, head.T, states.reshape(1, -1), class_of.reshape(1, -1), table.T
        )
        values = codes.astype(jnp.float32) * step[:, :, None, :] + base[:, :, None, :]
        log_probs = jnp.where(codes == FORBIDDEN, 0.0, values)
        return log_probs.reshape(-1, hidden.shape[0]).T, entropy.reshape(-1)

    in_specs = (P("rows", "vocab"), P(None, ("vocab", "rows")), P(), P("vocab"), P())
    out_specs = (P("rows", "vocab"), P("rows"))
    return jax.shard_map(on_device, mesh=mesh, in_specs=in_specs, out_specs=out_specs, check_vma=False)
```

```python
import functools

import jax
import jax.numpy as jnp
from jax import lax
from jax.experimental import pallas as pl
from jax.experimental.pallas import tpu as pltpu
from jax.sharding import PartitionSpec as P

MESH = pl.DeviceIdType.MESH
LANES = 128
BIG = 1e30
LEVELS = 65000.0
SHIFT = 32500
FORBIDDEN = -32768
MAX_CHUNKS = 11
BUFFERS = 3
FEW_BUFFERS = 2
PIECES = 4
SUB = 144
EXCHANGE_VMEM = 50 * 1024 * 1024
DECODE_VMEM = 24 * 1024 * 1024


def chunk_count(columns):
    for n in range(MAX_CHUNKS, 1, -1):
        if columns % n == 0 and (columns // n) % 16 == 0:
            return n
    return 1


def flip(v, bits):
    for bit in bits:
        size = 1 << bit
        v = v + size * (1 - 2 * lax.rem(lax.div(v, size), 2))
    return v


def subsets(bits):
    found = [()]
    for bit in bits:
        found = found + [s + (bit,) for s in found]
    return found


def exchange_kernel(
    nz, nv, hidden, head, states_in, class_of, table_in, codes_out, base_out, step_out, result,
    hid, buf, codes, banned, states, table, all_classes, classes, onehot, x, scale_rows, scale_land, stat_own, stat_land,
    z_send, z_recv, f_send, h_send, h_recv, own_sem, head_sem, c_send, c_recv, s_send, s_recv, loc_sem, t_send, t_recv,
    class_sem,
):
    rows, width = hidden.shape
    columns = head.shape[0]
    n = codes.shape[1]
    buffers = buf.shape[0]
    size = columns // n
    half = nz // 2
    piece = rows // PIECES
    steps = nv.bit_length() - 1
    z = lax.axis_index("rows")
    v = lax.axis_index("vocab")
    side = lax.div(z, half)
    passes = 2
    far_base = (1 - side) * half
    near_base = side * half

    def send(src, dst, ssem, rsem, zz, vv):
        return pltpu.make_async_remote_copy(
            src_ref=src, dst_ref=dst, send_sem=ssem, recv_sem=rsem, device_id=(zz, vv), device_id_type=MESH
        )

    def z_peer(j):
        return lax.rem(z + j, nz)

    def v_peer(j):
        return lax.rem(v + j, nv)

    barrier = pltpu.get_barrier_semaphore()
    for j in range(1, nz):
        pl.semaphore_signal(barrier, inc=1, device_id=(z_peer(j), v), device_id_type=MESH)
    for j in range(1, nv):
        pl.semaphore_signal(barrier, inc=1, device_id=(z, v_peer(j)), device_id_type=MESH)

    def head_copy(t):
        at = lax.rem(t, buffers)
        start = pl.multiple_of(lax.rem(t, n) * size, 16) if n > 1 else 0
        return pltpu.make_async_copy(head.at[pl.ds(start, size), :], buf.at[at], head_sem.at[at])

    small = [
        pltpu.make_async_copy(class_of, all_classes.at[0], class_sem.at[0]),
        pltpu.make_async_copy(states_in, states, class_sem.at[1]),
        pltpu.make_async_copy(table_in, table, class_sem.at[2]),
    ]
    for copy in small:
        copy.start()
    for t in range(min(buffers, passes * n)):
        head_copy(jnp.int32(t)).start()

    pl.semaphore_wait(barrier, nz - 1 + nv - 1)

    def slot(zz, p, vv):
        return hid.at[zz, pl.ds(p * piece, piece), pl.ds(pl.multiple_of(vv * width, width), width)]

    def own(p):
        return hidden.at[pl.ds(p * piece, piece), :]

    def far(k):
        return (1 - side) * (half + k) + side * (half - 1 - k)

    depth = (1 - side) * (half - 1 - z) + side * (z - half)
    inward = z + 1 - 2 * side
    outward = jnp.clip(z - 1 + 2 * side, 0, nz - 1)
    has_outward = depth < half - 1

    def near(e):
        return (1 - side) * (half - 1 - e) + side * (half + e)

    def own_inward(p):
        return send(own(p), slot(z, p, v), z_send.at[0, p], z_recv.at[z, p], inward, v)

    def own_outward(p):
        return send(own(p), slot(z, p, v), z_send.at[1, p], z_recv.at[z, p], outward, v)

    def onward(zz, p, target):
        return send(slot(zz, p, v), slot(zz, p, v), f_send.at[zz, p], z_recv.at[zz, p], target, v)

    def arrived(zz, p):
        onward(zz, p, z).wait_recv()

    for p in range(PIECES):
        own_inward(p).start()
    for p in range(PIECES):
        pltpu.make_async_copy(own(p), slot(z, p, v), own_sem.at[p]).start()

    def order(p):
        upper = list(range(1, steps))
        if p % 2:
            upper = upper[::-1]
        return upper + [0]

    def spread(q, zz, p, s):
        bits = order(p)
        partner = flip(v, [bits[s]])
        for m in subsets(bits[:s]):
            vv = flip(v, m)
            block = slot(zz, p, vv)
            send(block, block, h_send.at[q, p, s], h_recv.at[q, p, s], z, partner).start()

    def spread_step(q, p, s):
        block = hid.at[0, pl.ds(p * piece, piece), pl.ds(0, width << s)]
        return send(block, block, h_send.at[q, p, s], h_recv.at[q, p, s], z, v)

    for copy in small:
        copy.wait()

    for zz in range(nz):
        @pl.when(z == zz)
        def _(zz=zz):
            classes[:, pl.ds(0, columns)] = all_classes[:, zz * columns:(zz + 1) * columns]

    n_classes = onehot.shape[1]
    kinds = lax.broadcasted_iota(jnp.int32, (LANES, n_classes), 1)
    for b in range(-(-columns // LANES)):
        some = min(LANES, columns - b * LANES)
        line = classes[:, b * LANES:(b + 1) * LANES]
        turned = jnp.transpose(jnp.broadcast_to(line, (LANES, LANES)))
        wide = jnp.concatenate([turned] * (n_classes // LANES), axis=1)
        hot = jnp.where(wide == kinds, 1.0, 0.0).astype(jnp.bfloat16)
        onehot[b * LANES:b * LANES + some, :] = hot[:some]

    n_words, n_states = table.shape
    n_bytes = 4 * n_words
    packed = table[...]
    parts = [jnp.bitwise_and(jnp.right_shift(packed, 8 * b), 255) for b in range(4)]
    octets = jnp.concatenate(parts, axis=0).astype(jnp.float32).astype(jnp.bfloat16)
    which = lax.broadcasted_iota(jnp.int32, (n_states, rows), 0)
    bits8 = lax.broadcasted_iota(jnp.int32, (8, rows), 0)
    for g in range(nz):
        hot = jnp.where(which == states[:, g * rows:(g + 1) * rows], 1.0, 0.0).astype(jnp.bfloat16)
        found = jnp.dot(octets, hot, preferred_element_type=jnp.float32).astype(jnp.int32)
        blocks = []
        for w in range(n_words):
            for b in range(4):
                line = found[b * n_words + w:b * n_words + w + 1, :]
                bit = jnp.bitwise_and(jnp.right_shift(jnp.broadcast_to(line, (8, rows)), bits8), 1)
                blocks.append(jnp.where(bit > 0, 0.0, -BIG))
        banned[g] = jnp.concatenate(blocks, axis=0).astype(jnp.bfloat16)

    def running(g):
        return scale_rows.at[g, pl.ds(2 * n, 8), :]

    for g in range(nz):
        first = lax.broadcasted_iota(jnp.int32, (8, rows), 0) == 0
        scale_rows[g, 2 * n:2 * n + 8, :] = jnp.where(first, -BIG, 0.0)

    def far_arrive(k):
        for p in range(PIECES):
            arrived(far(k), p)

            @pl.when(has_outward)
            def _(p=p):
                onward(far(k), p, outward).start()

            spread(k, far(k), p, 0)

    def far_spread(k, s):
        for p in range(PIECES):
            spread_step(k, p, s - 1).wait_recv()
            if s < steps:
                spread(k, far(k), p, s)

    def from_outside():
        for e in range(1, half):
            @pl.when(e > depth)
            def _(e=e):
                for p in range(PIECES):
                    arrived(near(e), p)
                    onward(near(e), p, inward).start()

    def near_arrive():
        for e in range(half - 1):
            @pl.when(e < depth)
            def _(e=e):
                for p in range(PIECES):
                    arrived(near(e), p)

                    @pl.when(has_outward)
                    def _(p=p):
                        onward(near(e), p, outward).start()

        for p in range(PIECES):
            pltpu.make_async_copy(own(p), slot(z, p, v), own_sem.at[p]).wait()

    def near_spread(s):
        for e in range(half):
            for p in range(PIECES):
                if s > 0:
                    spread_step(half + e, p, s - 1).wait_recv()
                if s < steps:
                    spread(half + e, near(e), p, s)

    far_arrive(0)
    from_outside()
    for k in range(1, half):
        far_arrive(k)

    @pl.when(has_outward)
    def _():
        for p in range(PIECES):
            own_outward(p).start()

    for s in range(1, steps):
        for k in range(half):
            far_spread(k, s)
    near_arrive()
    near_spread(0)
    for k in range(half):
        far_spread(k, steps)

    def encode(g, i, lanes):
        values = x[:, lanes]
        high = jnp.max(values, axis=0, keepdims=True)
        low = jnp.min(jnp.where(values > -0.1 * BIG, values, BIG), axis=0, keepdims=True)
        gap = jnp.maximum(high - low, 1e-30)
        rate = LEVELS / gap
        total = jnp.zeros((1, rows), jnp.float32)
        weighted = jnp.zeros((1, rows), jnp.float32)
        for r in range(0, size, SUB):
            end = min(r + SUB, size)
            values = x[r:end, lanes]
            level = jnp.maximum((values - low) * rate + 0.5, float(FORBIDDEN + SHIFT))
            codes[g, i, r:end, :] = (level.astype(jnp.int32) - SHIFT).astype(jnp.int16)
            weights = jnp.exp(values - high)
            total = total + jnp.sum(weights, axis=0, keepdims=True)
            weighted = weighted + jnp.sum(weights * values, axis=0, keepdims=True)
        step = gap * (1.0 / LEVELS)
        scale_rows[g, pl.ds(i, 1), :] = low + SHIFT * step
        scale_rows[g, pl.ds(n + i, 1), :] = step
        old = scale_rows[g, 2 * n:2 * n + 3, :]
        peak = jnp.maximum(old[0:1], high)
        f0 = jnp.exp(old[0:1] - peak)
        f1 = jnp.exp(high - peak)
        scale_rows[g, 2 * n:2 * n + 1, :] = peak
        scale_rows[g, 2 * n + 1:2 * n + 2, :] = f0 * old[1:2] + f1 * total
        scale_rows[g, 2 * n + 2:2 * n + 3, :] = f0 * old[2:3] + f1 * weighted

    def code_copy(g, i):
        return send(codes.at[g, i], codes_out.at[z, i], c_send.at[g], c_recv.at[z], g, v)

    def scale_copy(g):
        return send(scale_rows.at[g], scale_land.at[z], s_send.at[g], s_recv.at[z], g, v)

    def run_pass(index, parts, events):
        def chunk_step(i, carry):
            t = index * n + i
            for at, event in events:
                @pl.when(i == min(at, n - 1))
                def _(event=event):
                    event()
            head_copy(t).wait()
            mine = onehot[pl.ds(pl.multiple_of(i * size, 16) if n > 1 else 0, size), :]
            for base, count, with_own in parts:
                weights = hid[pl.ds(base, count)].reshape(count * rows, hid.shape[2])
                got = lax.dot_general(
                    buf[lax.rem(t, buffers)], weights, (((1,), (1,)), ((), ())), preferred_element_type=jnp.float32
                )
                for j in range(count):
                    x[:, j * rows:(j + 1) * rows] = got[:, j * rows:(j + 1) * rows] + jnp.dot(
                        mine, banned[base + j], preferred_element_type=jnp.float32
                    )
                for j in range(count):
                    encode(base + j, i, slice(j * rows, (j + 1) * rows))
                for j in range(count):
                    g = base + j
                    if not with_own:
                        code_copy(g, i).start()
                    else:
                        @pl.when(g != z)
                        def _(g=g):
                            code_copy(g, i).start()

                        @pl.when(g == z)
                        def _(g=g):
                            pltpu.make_async_copy(codes.at[g, i], codes_out.at[z, i], loc_sem).start()

            @pl.when(t + buffers < passes * n)
            def _():
                head_copy(t + buffers).start()

            return carry

        lax.fori_loop(0, n, chunk_step, 0)
        for base, count, with_own in parts:
            for j in range(count):
                g = base + j
                if not with_own:
                    scale_copy(g).start()
                else:
                    @pl.when(g != z)
                    def _(g=g):
                        scale_copy(g).start()

    events = []
    for s in range(1, steps + 1):
        events.append(functools.partial(near_spread, s))
    run_pass(0, [(far_base, half, False)], list(zip([1, 5, 8] + [n - 1] * steps, events)))
    run_pass(1, [(near_base, half, True)], [])
    scale_land[z] = scale_rows[z]

    for j in range(1, nz):
        g = z_peer(j)
        send(scale_rows.at[g], scale_land.at[g], s_send.at[g], s_recv.at[g], z, v).wait_recv()

    def combine(ref, count, line):
        peaks, totals, weights = [
            jnp.concatenate([ref[q, line + k:line + k + 1, :] for q in range(count)], axis=0) for k in range(3)
        ]
        peak = jnp.max(peaks, axis=0, keepdims=True)
        factor = jnp.exp(peaks - peak)
        return (
            peak,
            jnp.sum(factor * totals, axis=0, keepdims=True),
            jnp.sum(factor * weights, axis=0, keepdims=True),
        )

    def stat_copy(j):
        return send(stat_own, stat_land.at[v], t_send.at[j], t_recv.at[v], z, v_peer(j))

    summed = jnp.concatenate([*combine(scale_land, nz, 2 * n), jnp.zeros((5, rows), jnp.float32)], axis=0)
    stat_own[...] = summed
    stat_land[v] = summed
    for j in range(1, nv):
        stat_copy(j).start()
    for j in range(1, nv):
        u = v_peer(j)
        send(stat_own, stat_land.at[u], t_send.at[j], t_recv.at[u], z, v).wait_recv()
    peak, total, weighted = combine(stat_land, nv, 0)
    norm = peak + jnp.log(total)
    result[...] = norm - weighted / total
    for g in range(nz):
        base_out[g] = scale_land[g, 0:n, :] - norm
        step_out[g] = scale_land[g, n:2 * n, :]

    for j in range(1, nz):
        g = z_peer(j)
        whole = send(codes.at[g], codes_out.at[g], c_send.at[g], c_recv.at[g], z, v)
        whole.wait_send()
        whole.wait_recv()
        scale_copy(g).wait_send()
    pltpu.make_async_copy(codes.at[z], codes_out.at[z], loc_sem).wait()
    for j in range(1, nv):
        stat_copy(j).wait_send()
    for p in range(PIECES):
        own_inward(p).wait_send()

        @pl.when(has_outward)
        def _(p=p):
            own_outward(p).wait_send()
            for k in range(half):
                onward(far(k), p, outward).wait_send()

        for e in range(half):
            @pl.when(e > depth)
            def _(e=e, p=p):
                onward(near(e), p, inward).wait_send()

            @pl.when(jnp.logical_and(e < depth, has_outward))
            def _(e=e, p=p):
                onward(near(e), p, outward).wait_send()

        for q in range(nz):
            for s in range(steps):
                spread_step(q, p, s).wait_send()


def exchange(nz, nv, hidden, head, states, class_of, table):
    rows, width = hidden.shape
    columns, depth = head.shape
    n = chunk_count(columns)
    size = columns // n
    lines = -(-(2 * n + 8) // 8) * 8
    buffers = BUFFERS if n > 1 else FEW_BUFFERS
    steps = nv.bit_length() - 1
    half = nz // 2
    padded = -(-columns // LANES) * LANES
    n_classes = table.shape[0] * 32
    vmem = pl.BlockSpec(memory_space=pltpu.VMEM)
    hbm = pl.BlockSpec(memory_space=pl.ANY)
    dma = pltpu.SemaphoreType.DMA
    return pl.pallas_call(
        functools.partial(exchange_kernel, nz, nv),
        out_shape=[
            pltpu.VMEM((nz, n, size, rows), jnp.int16),
            pltpu.VMEM((nz, n, rows), jnp.float32),
            pltpu.VMEM((nz, n, rows), jnp.float32),
            pltpu.VMEM((1, rows), jnp.float32),
        ],
        in_specs=[pl.BlockSpec(memory_space=pltpu.HBM)] * 5,
        out_specs=[hbm, vmem, vmem, vmem],
        scratch_shapes=[
            pltpu.VMEM((nz, rows, depth), jnp.bfloat16),
            pltpu.VMEM((buffers, size, depth), jnp.bfloat16),
            pltpu.VMEM((nz, n, size, rows), jnp.int16),
            pltpu.VMEM((nz, n_classes, rows), jnp.bfloat16),
            pltpu.VMEM(states.shape, jnp.int32),
            pltpu.VMEM(table.shape, jnp.int32),
            pltpu.VMEM((1, class_of.shape[0]), jnp.int32),
            pltpu.VMEM((1, padded), jnp.int32),
            pltpu.VMEM((columns, n_classes), jnp.bfloat16),
            pltpu.VMEM((size, half * rows), jnp.float32),
            pltpu.VMEM((nz, lines, rows), jnp.float32),
            pltpu.VMEM((nz, lines, rows), jnp.float32),
            pltpu.VMEM((8, rows), jnp.float32),
            pltpu.VMEM((nv, 8, rows), jnp.float32),
            dma((2, PIECES)),
            dma((nz, PIECES)),
            dma((nz, PIECES)),
            dma((nz, PIECES, steps)),
            dma((nz, PIECES, steps)),
            dma((PIECES,)),
            dma((buffers,)),
            dma((nz,)),
            dma((nz,)),
            dma((nz,)),
            dma((nz,)),
            dma,
            dma((nv,)),
            dma((nv,)),
            dma((3,)),
        ],
        compiler_params=pltpu.CompilerParams(
            collective_id=0, has_side_effects=True, vmem_limit_bytes=EXCHANGE_VMEM
        ),
    )(hidden, head, states, class_of, table)


def decode_kernel(codes, base, step, entropy, log_probs, entropy_out):
    i = pl.program_id(0)
    entropy_out[...] = entropy[...]
    for g in range(codes.shape[0]):
        level = codes[g, i].astype(jnp.int32)
        value = level.astype(jnp.float32) * step[g, pl.ds(i, 1), :] + base[g, pl.ds(i, 1), :]
        log_probs[g, 0] = jnp.where(level == FORBIDDEN, 0.0, value)


def decode(codes, base, step, entropy):
    nz, n, size, rows = codes.shape
    line = pl.BlockSpec((1, rows), lambda i: (0, 0))
    block = pl.BlockSpec((nz, 1, size, rows), lambda i: (0, i, 0, 0))
    return pl.pallas_call(
        decode_kernel,
        grid=(n,),
        in_specs=[pl.BlockSpec(memory_space=pltpu.VMEM)] * 4,
        out_specs=[block, line],
        out_shape=[
            jax.ShapeDtypeStruct(codes.shape, jnp.float32),
            jax.ShapeDtypeStruct((1, rows), jnp.float32),
        ],
        compiler_params=pltpu.CompilerParams(dimension_semantics=("arbitrary",), vmem_limit_bytes=DECODE_VMEM),
    )(codes, base, step, entropy)


def solution(mesh):
    nz, nv = mesh.shape["rows"], mesh.shape["vocab"]

    def on_device(hidden, head, states, class_of, table):
        coded = exchange(nz, nv, hidden, head.T, states.reshape(1, -1), class_of, table.T)
        log_probs, entropy = decode(*coded)
        return log_probs.reshape(-1, hidden.shape[0]).T, entropy.reshape(-1)

    in_specs = (P("rows", "vocab"), P(None, ("vocab", "rows")), P(), P("vocab"), P())
    out_specs = (P("rows", "vocab"), P("rows"))
    return jax.shard_map(on_device, mesh=mesh, in_specs=in_specs, out_specs=out_specs, check_vma=False)
```

```python
import functools

import jax
import jax.numpy as jnp
from jax import lax
from jax.experimental import pallas as pl
from jax.experimental.pallas import tpu as pltpu
from jax.sharding import PartitionSpec as P

MESH = pl.DeviceIdType.MESH
LANES = 128
BIG = 1e30
LEVELS = 65000.0
SHIFT = 32500
FORBIDDEN = -32768
MAX_CHUNKS = 9
BUFFERS = 3
FEW_BUFFERS = 2
PIECES = 4
SUB = 176
PACE = 3
EXCHANGE_VMEM = 50 * 1024 * 1024
DECODE_VMEM = 24 * 1024 * 1024


def chunk_count(columns):
    for n in range(MAX_CHUNKS, 1, -1):
        if columns % n == 0 and (columns // n) % 16 == 0:
            return n
    return 1


def flip(v, bits):
    for bit in bits:
        size = 1 << bit
        v = v + size * (1 - 2 * lax.rem(lax.div(v, size), 2))
    return v


def subsets(bits):
    found = [()]
    for bit in bits:
        found = found + [s + (bit,) for s in found]
    return found


def exchange_kernel(
    nz, nv, hidden, head, states_in, class_of, table_in, codes_out, base_out, step_out, result,
    hid, buf, codes, banned, states, table, all_classes, classes, onehot, x, scale_rows, scale_land, stat_own, stat_land,
    z_send, z_recv, f_send, h_send, h_recv, own_sem, head_sem, c_send, c_recv, s_send, s_recv, loc_sem, t_send, t_recv,
    class_sem,
):
    rows, width = hidden.shape
    columns = head.shape[0]
    n = codes.shape[1]
    buffers = buf.shape[0]
    size = columns // n
    half = nz // 2
    piece = rows // PIECES
    steps = nv.bit_length() - 1
    z = lax.axis_index("rows")
    v = lax.axis_index("vocab")
    side = lax.div(z, half)
    passes = 2
    far_base = (1 - side) * half
    near_base = side * half

    def send(src, dst, ssem, rsem, zz, vv):
        return pltpu.make_async_remote_copy(
            src_ref=src, dst_ref=dst, send_sem=ssem, recv_sem=rsem, device_id=(zz, vv), device_id_type=MESH
        )

    def z_peer(j):
        return lax.rem(z + j, nz)

    def v_peer(j):
        return lax.rem(v + j, nv)

    barrier = pltpu.get_barrier_semaphore()
    for j in range(1, nz):
        pl.semaphore_signal(barrier, inc=1, device_id=(z_peer(j), v), device_id_type=MESH)
    for j in range(1, nv):
        pl.semaphore_signal(barrier, inc=1, device_id=(z, v_peer(j)), device_id_type=MESH)

    def head_copy(t):
        at = lax.rem(t, buffers)
        start = pl.multiple_of(lax.rem(t, n) * size, 16) if n > 1 else 0
        return pltpu.make_async_copy(head.at[pl.ds(start, size), :], buf.at[at], head_sem.at[at])

    small = [
        pltpu.make_async_copy(class_of, all_classes.at[0], class_sem.at[0]),
        pltpu.make_async_copy(states_in, states, class_sem.at[1]),
        pltpu.make_async_copy(table_in, table, class_sem.at[2]),
    ]
    for copy in small:
        copy.start()
    for t in range(min(buffers, passes * n)):
        head_copy(jnp.int32(t)).start()

    pl.semaphore_wait(barrier, nz - 1 + nv - 1)

    def slot(zz, p, vv):
        return hid.at[zz, pl.ds(p * piece, piece), pl.ds(pl.multiple_of(vv * width, width), width)]

    def own(p):
        return hidden.at[pl.ds(p * piece, piece), :]

    def far(k):
        return (1 - side) * (half + k) + side * (half - 1 - k)

    depth = (1 - side) * (half - 1 - z) + side * (z - half)
    inward = z + 1 - 2 * side
    outward = jnp.clip(z - 1 + 2 * side, 0, nz - 1)
    has_outward = depth < half - 1

    def near(e):
        return (1 - side) * (half - 1 - e) + side * (half + e)

    def own_inward(p):
        return send(own(p), slot(z, p, v), z_send.at[0, p], z_recv.at[z, p], inward, v)

    def own_outward(p):
        return send(own(p), slot(z, p, v), z_send.at[1, p], z_recv.at[z, p], outward, v)

    def onward(zz, p, target):
        return send(slot(zz, p, v), slot(zz, p, v), f_send.at[zz, p], z_recv.at[zz, p], target, v)

    def arrived(zz, p):
        onward(zz, p, z).wait_recv()

    for p in range(PIECES):
        own_inward(p).start()
    for p in range(PIECES):
        pltpu.make_async_copy(own(p), slot(z, p, v), own_sem.at[p]).start()

    def order(p):
        upper = list(range(1, steps))
        if p % 2:
            upper = upper[::-1]
        return upper + [0]

    def spread(q, zz, p, s):
        bits = order(p)
        partner = flip(v, [bits[s]])
        for m in subsets(bits[:s]):
            vv = flip(v, m)
            block = slot(zz, p, vv)
            send(block, block, h_send.at[q, p, s], h_recv.at[q, p, s], z, partner).start()

    def spread_step(q, p, s):
        block = hid.at[0, pl.ds(p * piece, piece), pl.ds(0, width << s)]
        return send(block, block, h_send.at[q, p, s], h_recv.at[q, p, s], z, v)

    for copy in small:
        copy.wait()

    for zz in range(nz):
        @pl.when(z == zz)
        def _(zz=zz):
            classes[:, pl.ds(0, columns)] = all_classes[:, zz * columns:(zz + 1) * columns]

    n_classes = onehot.shape[1]
    kinds = lax.broadcasted_iota(jnp.int32, (LANES, n_classes), 1)
    for b in range(-(-columns // LANES)):
        some = min(LANES, columns - b * LANES)
        line = classes[:, b * LANES:(b + 1) * LANES]
        turned = jnp.transpose(jnp.broadcast_to(line, (LANES, LANES)))
        wide = jnp.concatenate([turned] * (n_classes // LANES), axis=1)
        hot = jnp.where(wide == kinds, 1.0, 0.0).astype(jnp.bfloat16)
        onehot[b * LANES:b * LANES + some, :] = hot[:some]

    n_words, n_states = table.shape
    n_bytes = 4 * n_words
    packed = table[...]
    parts = [jnp.bitwise_and(jnp.right_shift(packed, 8 * b), 255) for b in range(4)]
    octets = jnp.concatenate(parts, axis=0).astype(jnp.float32).astype(jnp.bfloat16)
    which = lax.broadcasted_iota(jnp.int32, (n_states, rows), 0)
    bits8 = lax.broadcasted_iota(jnp.int32, (8, rows), 0)
    for g in range(nz):
        hot = jnp.where(which == states[:, g * rows:(g + 1) * rows], 1.0, 0.0).astype(jnp.bfloat16)
        found = jnp.dot(octets, hot, preferred_element_type=jnp.float32).astype(jnp.int32)
        blocks = []
        for w in range(n_words):
            for b in range(4):
                line = found[b * n_words + w:b * n_words + w + 1, :]
                bit = jnp.bitwise_and(jnp.right_shift(jnp.broadcast_to(line, (8, rows)), bits8), 1)
                blocks.append(jnp.where(bit > 0, 0.0, -BIG))
        banned[g] = jnp.concatenate(blocks, axis=0).astype(jnp.bfloat16)

    def running(g):
        return scale_rows.at[g, pl.ds(2 * n, 8), :]

    for g in range(nz):
        first = lax.broadcasted_iota(jnp.int32, (8, rows), 0) == 0
        scale_rows[g, 2 * n:2 * n + 8, :] = jnp.where(first, -BIG, 0.0)

    def far_arrive(k):
        for p in range(PIECES):
            arrived(far(k), p)

            @pl.when(has_outward)
            def _(p=p):
                onward(far(k), p, outward).start()

            spread(k, far(k), p, 0)

    def far_spread(k, s):
        for p in range(PIECES):
            spread_step(k, p, s - 1).wait_recv()
            if s < steps:
                spread(k, far(k), p, s)

    def from_outside():
        for e in range(1, half):
            @pl.when(e > depth)
            def _(e=e):
                for p in range(PIECES):
                    arrived(near(e), p)
                    onward(near(e), p, inward).start()

    def near_arrive():
        for e in range(half - 1):
            @pl.when(e < depth)
            def _(e=e):
                for p in range(PIECES):
                    arrived(near(e), p)

                    @pl.when(has_outward)
                    def _(p=p):
                        onward(near(e), p, outward).start()

        for p in range(PIECES):
            pltpu.make_async_copy(own(p), slot(z, p, v), own_sem.at[p]).wait()

    def near_spread(s):
        for e in range(half):
            for p in range(PIECES):
                if s > 0:
                    spread_step(half + e, p, s - 1).wait_recv()
                if s < steps:
                    spread(half + e, near(e), p, s)

    far_arrive(0)
    from_outside()
    for k in range(half):
        if k > 0:
            far_arrive(k)
        if steps > 1:
            far_spread(k, 1)

    @pl.when(has_outward)
    def _():
        for p in range(PIECES):
            own_outward(p).start()

    for s in range(2, steps):
        for k in range(half):
            far_spread(k, s)
    for k in range(half):
        far_spread(k, steps)

    def encode(g, i, lanes):
        values = x[:, lanes]
        high = jnp.max(values, axis=0, keepdims=True)
        low = jnp.min(jnp.where(values > -0.1 * BIG, values, BIG), axis=0, keepdims=True)
        gap = jnp.maximum(high - low, 1e-30)
        rate = LEVELS / gap
        total = jnp.zeros((1, rows), jnp.float32)
        weighted = jnp.zeros((1, rows), jnp.float32)
        for r in range(0, size, SUB):
            end = min(r + SUB, size)
            values = x[r:end, lanes]
            level = jnp.maximum((values - low) * rate + 0.5, float(FORBIDDEN + SHIFT))
            codes[g, i, r:end, :] = (level.astype(jnp.int32) - SHIFT).astype(jnp.int16)
            weights = jnp.exp(values - high)
            total = total + jnp.sum(weights, axis=0, keepdims=True)
            weighted = weighted + jnp.sum(weights * values, axis=0, keepdims=True)
        step = gap * (1.0 / LEVELS)
        scale_rows[g, pl.ds(i, 1), :] = low + SHIFT * step
        scale_rows[g, pl.ds(n + i, 1), :] = step
        old = scale_rows[g, 2 * n:2 * n + 3, :]
        peak = jnp.maximum(old[0:1], high)
        f0 = jnp.exp(old[0:1] - peak)
        f1 = jnp.exp(high - peak)
        scale_rows[g, 2 * n:2 * n + 1, :] = peak
        scale_rows[g, 2 * n + 1:2 * n + 2, :] = f0 * old[1:2] + f1 * total
        scale_rows[g, 2 * n + 2:2 * n + 3, :] = f0 * old[2:3] + f1 * weighted

    def code_copy(g, i):
        return send(codes.at[g, i], codes_out.at[z, i], c_send.at[g], c_recv.at[z], g, v)

    def scale_copy(g):
        return send(scale_rows.at[g], scale_land.at[z], s_send.at[g], s_recv.at[z], g, v)

    def send_far(k):
        for j in range(half):
            code_copy(far_base + j, k).start()

    def run_pass(index, parts, events):
        def chunk_step(i, carry):
            t = index * n + i
            for at, event in events:
                @pl.when(i == min(at, n - 1))
                def _(event=event):
                    event()
            head_copy(t).wait()
            mine = onehot[pl.ds(pl.multiple_of(i * size, 16) if n > 1 else 0, size), :]
            for base, count, with_own in parts:
                weights = hid[pl.ds(base, count)].reshape(count * rows, hid.shape[2])
                got = lax.dot_general(
                    buf[lax.rem(t, buffers)], weights, (((1,), (1,)), ((), ())), preferred_element_type=jnp.float32
                )
                for j in range(count):
                    x[:, j * rows:(j + 1) * rows] = got[:, j * rows:(j + 1) * rows] + jnp.dot(
                        mine, banned[base + j], preferred_element_type=jnp.float32
                    )
                for j in range(count):
                    encode(base + j, i, slice(j * rows, (j + 1) * rows))
                for j in range(count):
                    g = base + j
                    if with_own:
                        @pl.when(g != z)
                        def _(g=g):
                            code_copy(g, i).start()

                        @pl.when(g == z)
                        def _(g=g):
                            pltpu.make_async_copy(codes.at[g, i], codes_out.at[z, i], loc_sem).start()

            @pl.when(t + buffers < passes * n)
            def _():
                head_copy(t + buffers).start()

            late = lax.div(t - 1, PACE) + 1
            k = jnp.where(t < 2, t, late)
            due = jnp.logical_or(t < 2, jnp.logical_and(t > PACE, lax.rem(t - 1, PACE) == 0))

            @pl.when(jnp.logical_and(due, k < n))
            def _():
                send_far(k)

            return carry

        lax.fori_loop(0, n, chunk_step, 0)
        for base, count, with_own in parts:
            for j in range(count):
                g = base + j
                if not with_own:
                    scale_copy(g).start()
                else:
                    @pl.when(g != z)
                    def _(g=g):
                        scale_copy(g).start()

    def near_start():
        near_arrive()
        near_spread(0)

    events = [near_start]
    for s in range(1, steps + 1):
        events.append(functools.partial(near_spread, s))
    run_pass(0, [(far_base, half, False)], list(zip([0, 2, 5, 7] + [n - 1] * steps, events)))
    run_pass(1, [(near_base, half, True)], [])

    def send_rest(k, carry):
        send_far(k)
        return carry

    lax.fori_loop(min(n, 2 + (2 * n - 2) // PACE), n, send_rest, 0)
    scale_land[z] = scale_rows[z]

    for j in range(1, nz):
        g = z_peer(j)
        send(scale_rows.at[g], scale_land.at[g], s_send.at[g], s_recv.at[g], z, v).wait_recv()

    def combine(ref, count, line):
        peaks, totals, weights = [
            jnp.concatenate([ref[q, line + k:line + k + 1, :] for q in range(count)], axis=0) for k in range(3)
        ]
        peak = jnp.max(peaks, axis=0, keepdims=True)
        factor = jnp.exp(peaks - peak)
        return (
            peak,
            jnp.sum(factor * totals, axis=0, keepdims=True),
            jnp.sum(factor * weights, axis=0, keepdims=True),
        )

    def stat_copy(j):
        return send(stat_own, stat_land.at[v], t_send.at[j], t_recv.at[v], z, v_peer(j))

    summed = jnp.concatenate([*combine(scale_land, nz, 2 * n), jnp.zeros((5, rows), jnp.float32)], axis=0)
    stat_own[...] = summed
    stat_land[v] = summed
    for j in range(1, nv):
        stat_copy(j).start()
    for j in range(1, nv):
        u = v_peer(j)
        send(stat_own, stat_land.at[u], t_send.at[j], t_recv.at[u], z, v).wait_recv()
    peak, total, weighted = combine(stat_land, nv, 0)
    norm = peak + jnp.log(total)
    result[...] = norm - weighted / total
    for g in range(nz):
        base_out[g] = scale_land[g, 0:n, :] - norm
        step_out[g] = scale_land[g, n:2 * n, :]

    for j in range(1, nz):
        g = z_peer(j)
        whole = send(codes.at[g], codes_out.at[g], c_send.at[g], c_recv.at[g], z, v)
        whole.wait_send()
        whole.wait_recv()
        scale_copy(g).wait_send()
    pltpu.make_async_copy(codes.at[z], codes_out.at[z], loc_sem).wait()
    for j in range(1, nv):
        stat_copy(j).wait_send()
    for p in range(PIECES):
        own_inward(p).wait_send()

        @pl.when(has_outward)
        def _(p=p):
            own_outward(p).wait_send()
            for k in range(half):
                onward(far(k), p, outward).wait_send()

        for e in range(half):
            @pl.when(e > depth)
            def _(e=e, p=p):
                onward(near(e), p, inward).wait_send()

            @pl.when(jnp.logical_and(e < depth, has_outward))
            def _(e=e, p=p):
                onward(near(e), p, outward).wait_send()

        for q in range(nz):
            for s in range(steps):
                spread_step(q, p, s).wait_send()


def exchange(nz, nv, hidden, head, states, class_of, table):
    rows, width = hidden.shape
    columns, depth = head.shape
    n = chunk_count(columns)
    size = columns // n
    lines = -(-(2 * n + 8) // 8) * 8
    buffers = BUFFERS if n > 1 else FEW_BUFFERS
    steps = nv.bit_length() - 1
    half = nz // 2
    padded = -(-columns // LANES) * LANES
    n_classes = table.shape[0] * 32
    vmem = pl.BlockSpec(memory_space=pltpu.VMEM)
    hbm = pl.BlockSpec(memory_space=pl.ANY)
    dma = pltpu.SemaphoreType.DMA
    return pl.pallas_call(
        functools.partial(exchange_kernel, nz, nv),
        out_shape=[
            pltpu.VMEM((nz, n, size, rows), jnp.int16),
            pltpu.VMEM((nz, n, rows), jnp.float32),
            pltpu.VMEM((nz, n, rows), jnp.float32),
            pltpu.VMEM((1, rows), jnp.float32),
        ],
        in_specs=[pl.BlockSpec(memory_space=pltpu.HBM)] * 5,
        out_specs=[hbm, vmem, vmem, vmem],
        scratch_shapes=[
            pltpu.VMEM((nz, rows, depth), jnp.bfloat16),
            pltpu.VMEM((buffers, size, depth), jnp.bfloat16),
            pltpu.VMEM((nz, n, size, rows), jnp.int16),
            pltpu.VMEM((nz, n_classes, rows), jnp.bfloat16),
            pltpu.VMEM(states.shape, jnp.int32),
            pltpu.VMEM(table.shape, jnp.int32),
            pltpu.VMEM((1, class_of.shape[0]), jnp.int32),
            pltpu.VMEM((1, padded), jnp.int32),
            pltpu.VMEM((columns, n_classes), jnp.bfloat16),
            pltpu.VMEM((size, half * rows), jnp.float32),
            pltpu.VMEM((nz, lines, rows), jnp.float32),
            pltpu.VMEM((nz, lines, rows), jnp.float32),
            pltpu.VMEM((8, rows), jnp.float32),
            pltpu.VMEM((nv, 8, rows), jnp.float32),
            dma((2, PIECES)),
            dma((nz, PIECES)),
            dma((nz, PIECES)),
            dma((nz, PIECES, steps)),
            dma((nz, PIECES, steps)),
            dma((PIECES,)),
            dma((buffers,)),
            dma((nz,)),
            dma((nz,)),
            dma((nz,)),
            dma((nz,)),
            dma,
            dma((nv,)),
            dma((nv,)),
            dma((3,)),
        ],
        compiler_params=pltpu.CompilerParams(
            collective_id=0, has_side_effects=True, vmem_limit_bytes=EXCHANGE_VMEM
        ),
    )(hidden, head, states, class_of, table)


def decode_kernel(codes, base, step, entropy, log_probs, entropy_out):
    i = pl.program_id(0)
    entropy_out[...] = entropy[...]
    for g in range(codes.shape[0]):
        level = codes[g, i].astype(jnp.int32)
        value = level.astype(jnp.float32) * step[g, pl.ds(i, 1), :] + base[g, pl.ds(i, 1), :]
        log_probs[g, 0] = jnp.where(level == FORBIDDEN, 0.0, value)


def decode(codes, base, step, entropy):
    nz, n, size, rows = codes.shape
    line = pl.BlockSpec((1, rows), lambda i: (0, 0))
    block = pl.BlockSpec((nz, 1, size, rows), lambda i: (0, i, 0, 0))
    return pl.pallas_call(
        decode_kernel,
        grid=(n,),
        in_specs=[pl.BlockSpec(memory_space=pltpu.VMEM)] * 4,
        out_specs=[block, line],
        out_shape=[
            jax.ShapeDtypeStruct(codes.shape, jnp.float32),
            jax.ShapeDtypeStruct((1, rows), jnp.float32),
        ],
        compiler_params=pltpu.CompilerParams(dimension_semantics=("arbitrary",), vmem_limit_bytes=DECODE_VMEM),
    )(codes, base, step, entropy)


def solution(mesh):
    nz, nv = mesh.shape["rows"], mesh.shape["vocab"]

    def on_device(hidden, head, states, class_of, table):
        coded = exchange(nz, nv, hidden, head.T, states.reshape(1, -1), class_of, table.T)
        log_probs, entropy = decode(*coded)
        return log_probs.reshape(-1, hidden.shape[0]).T, entropy.reshape(-1)

    in_specs = (P("rows", "vocab"), P(None, ("vocab", "rows")), P(), P("vocab"), P())
    out_specs = (P("rows", "vocab"), P("rows"))
    return jax.shard_map(on_device, mesh=mesh, in_specs=in_specs, out_specs=out_specs, check_vma=False)
```

```python
import functools

import jax
import jax.numpy as jnp
from jax import lax
from jax.experimental import pallas as pl
from jax.experimental.pallas import tpu as pltpu
from jax.sharding import PartitionSpec as P

MESH = pl.DeviceIdType.MESH
LANES = 128
BIG = 1e30
LEVELS = 65000.0
SHIFT = 32500
FORBIDDEN = -32768
MAX_CHUNKS = 9
BUFFERS = 3
FEW_BUFFERS = 2
PIECES = 4
SUB = 176
PACE = 3
EARLY = 1
EXCHANGE_VMEM = 50 * 1024 * 1024
DECODE_VMEM = 24 * 1024 * 1024


def chunk_count(columns):
    for n in range(MAX_CHUNKS, 1, -1):
        if columns % n == 0 and (columns // n) % 16 == 0:
            return n
    return 1


def flip(v, bits):
    for bit in bits:
        size = 1 << bit
        v = v + size * (1 - 2 * lax.rem(lax.div(v, size), 2))
    return v


def subsets(bits):
    found = [()]
    for bit in bits:
        found = found + [s + (bit,) for s in found]
    return found


def exchange_kernel(
    nz, nv, hidden, head, states_in, class_of, table_in, codes_out, base_out, step_out, result,
    hid, buf, codes, banned, states, table, all_classes, classes, onehot, x, scale_rows, scale_land, stat_own, stat_land,
    z_send, z_recv, f_send, h_send, h_recv, own_sem, head_sem, c_send, c_recv, s_send, s_recv, loc_sem, t_send, t_recv,
    class_sem,
):
    rows, width = hidden.shape
    columns = head.shape[0]
    n = codes.shape[1]
    buffers = buf.shape[0]
    size = columns // n
    half = nz // 2
    piece = rows // PIECES
    steps = nv.bit_length() - 1
    z = lax.axis_index("rows")
    v = lax.axis_index("vocab")
    side = lax.div(z, half)
    passes = 2
    early = min(EARLY, n) if half > 1 else 0
    far_base = (1 - side) * half
    near_base = side * half

    def send(src, dst, ssem, rsem, zz, vv):
        return pltpu.make_async_remote_copy(
            src_ref=src, dst_ref=dst, send_sem=ssem, recv_sem=rsem, device_id=(zz, vv), device_id_type=MESH
        )

    def z_peer(j):
        return lax.rem(z + j, nz)

    def v_peer(j):
        return lax.rem(v + j, nv)

    barrier = pltpu.get_barrier_semaphore()
    for j in range(1, nz):
        pl.semaphore_signal(barrier, inc=1, device_id=(z_peer(j), v), device_id_type=MESH)
    for j in range(1, nv):
        pl.semaphore_signal(barrier, inc=1, device_id=(z, v_peer(j)), device_id_type=MESH)

    def head_copy(t):
        at = lax.rem(t, buffers)
        start = pl.multiple_of(lax.rem(t, n) * size, 16) if n > 1 else 0
        return pltpu.make_async_copy(head.at[pl.ds(start, size), :], buf.at[at], head_sem.at[at])

    small = [
        pltpu.make_async_copy(class_of, all_classes.at[0], class_sem.at[0]),
        pltpu.make_async_copy(states_in, states, class_sem.at[1]),
        pltpu.make_async_copy(table_in, table, class_sem.at[2]),
    ]
    for copy in small:
        copy.start()
    for t in range(min(buffers, passes * n)):
        head_copy(jnp.int32(t)).start()

    pl.semaphore_wait(barrier, nz - 1 + nv - 1)

    def slot(zz, p, vv):
        return hid.at[zz, pl.ds(p * piece, piece), pl.ds(pl.multiple_of(vv * width, width), width)]

    def own(p):
        return hidden.at[pl.ds(p * piece, piece), :]

    def far(k):
        return (1 - side) * (half + k) + side * (half - 1 - k)

    depth = (1 - side) * (half - 1 - z) + side * (z - half)
    inward = z + 1 - 2 * side
    outward = jnp.clip(z - 1 + 2 * side, 0, nz - 1)
    has_outward = depth < half - 1

    def near(e):
        return (1 - side) * (half - 1 - e) + side * (half + e)

    def own_inward(p):
        return send(own(p), slot(z, p, v), z_send.at[0, p], z_recv.at[z, p], inward, v)

    def own_outward(p):
        return send(own(p), slot(z, p, v), z_send.at[1, p], z_recv.at[z, p], outward, v)

    def onward(zz, p, target):
        return send(slot(zz, p, v), slot(zz, p, v), f_send.at[zz, p], z_recv.at[zz, p], target, v)

    def arrived(zz, p):
        onward(zz, p, z).wait_recv()

    for p in range(PIECES):
        own_inward(p).start()
    for p in range(PIECES):
        pltpu.make_async_copy(own(p), slot(z, p, v), own_sem.at[p]).start()

    def order(p):
        upper = list(range(1, steps))
        if p % 2:
            upper = upper[::-1]
        return upper + [0]

    def spread(q, zz, p, s):
        bits = order(p)
        partner = flip(v, [bits[s]])
        for m in subsets(bits[:s]):
            vv = flip(v, m)
            block = slot(zz, p, vv)
            send(block, block, h_send.at[q, p, s], h_recv.at[q, p, s], z, partner).start()

    def spread_step(q, p, s):
        block = hid.at[0, pl.ds(p * piece, piece), pl.ds(0, width << s)]
        return send(block, block, h_send.at[q, p, s], h_recv.at[q, p, s], z, v)

    for copy in small:
        copy.wait()

    for zz in range(nz):
        @pl.when(z == zz)
        def _(zz=zz):
            classes[:, pl.ds(0, columns)] = all_classes[:, zz * columns:(zz + 1) * columns]

    n_classes = onehot.shape[1]
    kinds = lax.broadcasted_iota(jnp.int32, (LANES, n_classes), 1)
    for b in range(-(-columns // LANES)):
        some = min(LANES, columns - b * LANES)
        line = classes[:, b * LANES:(b + 1) * LANES]
        turned = jnp.transpose(jnp.broadcast_to(line, (LANES, LANES)))
        wide = jnp.concatenate([turned] * (n_classes // LANES), axis=1)
        hot = jnp.where(wide == kinds, 1.0, 0.0).astype(jnp.bfloat16)
        onehot[b * LANES:b * LANES + some, :] = hot[:some]

    n_words, n_states = table.shape
    n_bytes = 4 * n_words
    packed = table[...]
    parts = [jnp.bitwise_and(jnp.right_shift(packed, 8 * b), 255) for b in range(4)]
    octets = jnp.concatenate(parts, axis=0).astype(jnp.float32).astype(jnp.bfloat16)
    which = lax.broadcasted_iota(jnp.int32, (n_states, rows), 0)
    bits8 = lax.broadcasted_iota(jnp.int32, (8, rows), 0)
    for g in range(nz):
        hot = jnp.where(which == states[:, g * rows:(g + 1) * rows], 1.0, 0.0).astype(jnp.bfloat16)
        found = jnp.dot(octets, hot, preferred_element_type=jnp.float32).astype(jnp.int32)
        blocks = []
        for w in range(n_words):
            for b in range(4):
                line = found[b * n_words + w:b * n_words + w + 1, :]
                bit = jnp.bitwise_and(jnp.right_shift(jnp.broadcast_to(line, (8, rows)), bits8), 1)
                blocks.append(jnp.where(bit > 0, 0.0, -BIG))
        banned[g] = jnp.concatenate(blocks, axis=0).astype(jnp.bfloat16)

    def running(g):
        return scale_rows.at[g, pl.ds(2 * n, 8), :]

    for g in range(nz):
        first = lax.broadcasted_iota(jnp.int32, (8, rows), 0) == 0
        scale_rows[g, 2 * n:2 * n + 8, :] = jnp.where(first, -BIG, 0.0)

    def far_arrive(k):
        for p in range(PIECES):
            arrived(far(k), p)

            @pl.when(has_outward)
            def _(p=p):
                onward(far(k), p, outward).start()

            spread(k, far(k), p, 0)

    def far_spread(k, s):
        for p in range(PIECES):
            spread_step(k, p, s - 1).wait_recv()
            if s < steps:
                spread(k, far(k), p, s)

    def from_outside():
        for e in range(1, half):
            @pl.when(e > depth)
            def _(e=e):
                for p in range(PIECES):
                    arrived(near(e), p)
                    onward(near(e), p, inward).start()

    def near_arrive():
        for e in range(half - 1):
            @pl.when(e < depth)
            def _(e=e):
                for p in range(PIECES):
                    arrived(near(e), p)

                    @pl.when(has_outward)
                    def _(p=p):
                        onward(near(e), p, outward).start()

        for p in range(PIECES):
            pltpu.make_async_copy(own(p), slot(z, p, v), own_sem.at[p]).wait()

    def near_spread(s):
        for e in range(half):
            for p in range(PIECES):
                if s > 0:
                    spread_step(half + e, p, s - 1).wait_recv()
                if s < steps:
                    spread(half + e, near(e), p, s)

    far_arrive(0)
    from_outside()
    for k in range(half):
        if k > 0:
            far_arrive(k)
        if steps > 1:
            far_spread(k, 1)

    @pl.when(has_outward)
    def _():
        for p in range(PIECES):
            own_outward(p).start()

    def encode(g, i, lanes):
        values = x[:, lanes]
        high = jnp.max(values, axis=0, keepdims=True)
        low = jnp.min(jnp.where(values > -0.1 * BIG, values, BIG), axis=0, keepdims=True)
        gap = jnp.maximum(high - low, 1e-30)
        rate = LEVELS / gap
        total = jnp.zeros((1, rows), jnp.float32)
        weighted = jnp.zeros((1, rows), jnp.float32)
        for r in range(0, size, SUB):
            end = min(r + SUB, size)
            values = x[r:end, lanes]
            level = jnp.maximum((values - low) * rate + 0.5, float(FORBIDDEN + SHIFT))
            codes[g, i, r:end, :] = (level.astype(jnp.int32) - SHIFT).astype(jnp.int16)
            weights = jnp.exp(values - high)
            total = total + jnp.sum(weights, axis=0, keepdims=True)
            weighted = weighted + jnp.sum(weights * values, axis=0, keepdims=True)
        step = gap * (1.0 / LEVELS)
        scale_rows[g, pl.ds(i, 1), :] = low + SHIFT * step
        scale_rows[g, pl.ds(n + i, 1), :] = step
        old = scale_rows[g, 2 * n:2 * n + 3, :]
        peak = jnp.maximum(old[0:1], high)
        f0 = jnp.exp(old[0:1] - peak)
        f1 = jnp.exp(high - peak)
        scale_rows[g, 2 * n:2 * n + 1, :] = peak
        scale_rows[g, 2 * n + 1:2 * n + 2, :] = f0 * old[1:2] + f1 * total
        scale_rows[g, 2 * n + 2:2 * n + 3, :] = f0 * old[2:3] + f1 * weighted

    def code_copy(g, i):
        return send(codes.at[g, i], codes_out.at[z, i], c_send.at[g], c_recv.at[z], g, v)

    def scale_copy(g):
        return send(scale_rows.at[g], scale_land.at[z], s_send.at[g], s_recv.at[z], g, v)

    def send_far(k):
        for j in range(half):
            code_copy(far_base + j, k).start()

    def send_far_rest(k):
        for j in range(1, half):
            code_copy(far(j), k).start()

    def multiply(i, at, base, count):
        start = i * size if isinstance(i, int) else pl.multiple_of(i * size, 16)
        mine = onehot[pl.ds(start if n > 1 else 0, size), :]
        weights = hid[pl.ds(base, count)].reshape(count * rows, hid.shape[2])
        got = lax.dot_general(buf[at], weights, (((1,), (1,)), ((), ())), preferred_element_type=jnp.float32)
        for j in range(count):
            x[:, j * rows:(j + 1) * rows] = got[:, j * rows:(j + 1) * rows] + jnp.dot(
                mine, banned[base + j], preferred_element_type=jnp.float32
            )
        for j in range(count):
            encode(base + j, i, slice(j * rows, (j + 1) * rows))

    def run_pass(index, parts, events):
        def chunk_step(i, carry):
            t = index * n + i
            for at, event in events:
                @pl.when(i == min(at, n - 1))
                def _(event=event):
                    event()
            if index == 0 and early:
                @pl.when(i >= early)
                def _():
                    head_copy(t).wait()
            else:
                head_copy(t).wait()
            at = lax.rem(t, buffers)
            for base, count, with_own in parts:
                if with_own or not early:
                    multiply(i, at, base, count)
                else:
                    @pl.when(i < early)
                    def _():
                        multiply(i, at, (1 - side) * (half + 1), half - 1)

                    if early < n:
                        @pl.when(i >= early)
                        def _(base=base, count=count):
                            multiply(i, at, base, count)
                for j in range(count):
                    g = base + j
                    if with_own:
                        @pl.when(g != z)
                        def _(g=g):
                            code_copy(g, i).start()

                        @pl.when(g == z)
                        def _(g=g):
                            pltpu.make_async_copy(codes.at[g, i], codes_out.at[z, i], loc_sem).start()

            @pl.when(t + buffers < passes * n)
            def _():
                head_copy(t + buffers).start()

            late = lax.div(t - 1, PACE) + 1
            k = jnp.where(t < 2, t, late)
            due = jnp.logical_or(t < 2, jnp.logical_and(t > PACE, lax.rem(t - 1, PACE) == 0))

            due = jnp.logical_and(due, k < n)

            @pl.when(jnp.logical_and(due, k < early))
            def _():
                send_far_rest(k)

            @pl.when(jnp.logical_and(due, k >= early))
            def _():
                send_far(k)

            return carry

        lax.fori_loop(0, n, chunk_step, 0)
        for base, count, with_own in parts:
            for j in range(count):
                g = base + j
                if not with_own:
                    scale_copy(g).start()
                else:
                    @pl.when(g != z)
                    def _(g=g):
                        scale_copy(g).start()

    for s in range(2, steps + 1):
        far_spread(0, s)
    for i in range(early):
        head_copy(jnp.int32(i)).wait()
        multiply(i, i, far(0), 1)
        code_copy(far(0), i).start()
    for s in range(2, steps + 1):
        for k in range(1, half):
            far_spread(k, s)

    def near_start():
        near_arrive()
        near_spread(0)

    events = [near_start]
    for s in range(1, steps + 1):
        events.append(functools.partial(near_spread, s))
    run_pass(0, [(far_base, half, False)], list(zip([0, 2, 5, 7] + [n - 1] * steps, events)))
    run_pass(1, [(near_base, half, True)], [])

    def send_rest(k, carry):
        send_far(k)
        return carry

    lax.fori_loop(min(n, 2 + (2 * n - 2) // PACE), n, send_rest, 0)
    scale_land[z] = scale_rows[z]

    for j in range(1, nz):
        g = z_peer(j)
        send(scale_rows.at[g], scale_land.at[g], s_send.at[g], s_recv.at[g], z, v).wait_recv()

    def combine(ref, count, line):
        peaks, totals, weights = [
            jnp.concatenate([ref[q, line + k:line + k + 1, :] for q in range(count)], axis=0) for k in range(3)
        ]
        peak = jnp.max(peaks, axis=0, keepdims=True)
        factor = jnp.exp(peaks - peak)
        return (
            peak,
            jnp.sum(factor * totals, axis=0, keepdims=True),
            jnp.sum(factor * weights, axis=0, keepdims=True),
        )

    def stat_copy(j):
        return send(stat_own, stat_land.at[v], t_send.at[j], t_recv.at[v], z, v_peer(j))

    summed = jnp.concatenate([*combine(scale_land, nz, 2 * n), jnp.zeros((5, rows), jnp.float32)], axis=0)
    stat_own[...] = summed
    stat_land[v] = summed
    for j in range(1, nv):
        stat_copy(j).start()
    for j in range(1, nv):
        u = v_peer(j)
        send(stat_own, stat_land.at[u], t_send.at[j], t_recv.at[u], z, v).wait_recv()
    peak, total, weighted = combine(stat_land, nv, 0)
    norm = peak + jnp.log(total)
    result[...] = norm - weighted / total
    for g in range(nz):
        base_out[g] = scale_land[g, 0:n, :] - norm
        step_out[g] = scale_land[g, n:2 * n, :]

    for j in range(1, nz):
        g = z_peer(j)
        whole = send(codes.at[g], codes_out.at[g], c_send.at[g], c_recv.at[g], z, v)
        whole.wait_send()
        whole.wait_recv()
        scale_copy(g).wait_send()
    pltpu.make_async_copy(codes.at[z], codes_out.at[z], loc_sem).wait()
    for j in range(1, nv):
        stat_copy(j).wait_send()
    for p in range(PIECES):
        own_inward(p).wait_send()

        @pl.when(has_outward)
        def _(p=p):
            own_outward(p).wait_send()
            for k in range(half):
                onward(far(k), p, outward).wait_send()

        for e in range(half):
            @pl.when(e > depth)
            def _(e=e, p=p):
                onward(near(e), p, inward).wait_send()

            @pl.when(jnp.logical_and(e < depth, has_outward))
            def _(e=e, p=p):
                onward(near(e), p, outward).wait_send()

        for q in range(nz):
            for s in range(steps):
                spread_step(q, p, s).wait_send()


def exchange(nz, nv, hidden, head, states, class_of, table):
    rows, width = hidden.shape
    columns, depth = head.shape
    n = chunk_count(columns)
    size = columns // n
    lines = -(-(2 * n + 8) // 8) * 8
    buffers = BUFFERS if n > 1 else FEW_BUFFERS
    steps = nv.bit_length() - 1
    half = nz // 2
    padded = -(-columns // LANES) * LANES
    n_classes = table.shape[0] * 32
    vmem = pl.BlockSpec(memory_space=pltpu.VMEM)
    hbm = pl.BlockSpec(memory_space=pl.ANY)
    dma = pltpu.SemaphoreType.DMA
    return pl.pallas_call(
        functools.partial(exchange_kernel, nz, nv),
        out_shape=[
            pltpu.VMEM((nz, n, size, rows), jnp.int16),
            pltpu.VMEM((nz, n, rows), jnp.float32),
            pltpu.VMEM((nz, n, rows), jnp.float32),
            pltpu.VMEM((1, rows), jnp.float32),
        ],
        in_specs=[pl.BlockSpec(memory_space=pltpu.HBM)] * 5,
        out_specs=[hbm, vmem, vmem, vmem],
        scratch_shapes=[
            pltpu.VMEM((nz, rows, depth), jnp.bfloat16),
            pltpu.VMEM((buffers, size, depth), jnp.bfloat16),
            pltpu.VMEM((nz, n, size, rows), jnp.int16),
            pltpu.VMEM((nz, n_classes, rows), jnp.bfloat16),
            pltpu.VMEM(states.shape, jnp.int32),
            pltpu.VMEM(table.shape, jnp.int32),
            pltpu.VMEM((1, class_of.shape[0]), jnp.int32),
            pltpu.VMEM((1, padded), jnp.int32),
            pltpu.VMEM((columns, n_classes), jnp.bfloat16),
            pltpu.VMEM((size, half * rows), jnp.float32),
            pltpu.VMEM((nz, lines, rows), jnp.float32),
            pltpu.VMEM((nz, lines, rows), jnp.float32),
            pltpu.VMEM((8, rows), jnp.float32),
            pltpu.VMEM((nv, 8, rows), jnp.float32),
            dma((2, PIECES)),
            dma((nz, PIECES)),
            dma((nz, PIECES)),
            dma((nz, PIECES, steps)),
            dma((nz, PIECES, steps)),
            dma((PIECES,)),
            dma((buffers,)),
            dma((nz,)),
            dma((nz,)),
            dma((nz,)),
            dma((nz,)),
            dma,
            dma((nv,)),
            dma((nv,)),
            dma((3,)),
        ],
        compiler_params=pltpu.CompilerParams(
            collective_id=0, has_side_effects=True, vmem_limit_bytes=EXCHANGE_VMEM
        ),
    )(hidden, head, states, class_of, table)


def decode_kernel(codes, base, step, entropy, log_probs, entropy_out):
    i = pl.program_id(0)
    entropy_out[...] = entropy[...]
    for g in range(codes.shape[0]):
        level = codes[g, i].astype(jnp.int32)
        value = level.astype(jnp.float32) * step[g, pl.ds(i, 1), :] + base[g, pl.ds(i, 1), :]
        log_probs[g, 0] = jnp.where(level == FORBIDDEN, 0.0, value)


def decode(codes, base, step, entropy):
    nz, n, size, rows = codes.shape
    line = pl.BlockSpec((1, rows), lambda i: (0, 0))
    block = pl.BlockSpec((nz, 1, size, rows), lambda i: (0, i, 0, 0))
    return pl.pallas_call(
        decode_kernel,
        grid=(n,),
        in_specs=[pl.BlockSpec(memory_space=pltpu.VMEM)] * 4,
        out_specs=[block, line],
        out_shape=[
            jax.ShapeDtypeStruct(codes.shape, jnp.float32),
            jax.ShapeDtypeStruct((1, rows), jnp.float32),
        ],
        compiler_params=pltpu.CompilerParams(dimension_semantics=("arbitrary",), vmem_limit_bytes=DECODE_VMEM),
    )(codes, base, step, entropy)


def solution(mesh):
    nz, nv = mesh.shape["rows"], mesh.shape["vocab"]

    def on_device(hidden, head, states, class_of, table):
        coded = exchange(nz, nv, hidden, head.T, states.reshape(1, -1), class_of, table.T)
        log_probs, entropy = decode(*coded)
        return log_probs.reshape(-1, hidden.shape[0]).T, entropy.reshape(-1)

    in_specs = (P("rows", "vocab"), P(None, ("vocab", "rows")), P(), P("vocab"), P())
    out_specs = (P("rows", "vocab"), P("rows"))
    return jax.shard_map(on_device, mesh=mesh, in_specs=in_specs, out_specs=out_specs, check_vma=False)
```
